128 devices in a mesh: tm: 8 (over x, z_hi), space: 16 (over y, z_lo, core).
Axes of the slice: x: 4, y: 4, z: 4 (z_hi: 2, z_lo: 2; z = z_hi * 2 + z_lo), core: 2. Of those that a mesh axis runs over, the one named last changes fastest.
Arguments:
- left_modes: bfloat16 [8, 2, 256, 32768], P('tm', None, None, 'space'), may hold values from -6 to 6
- right_modes: bfloat16 [8, 2, 256, 32768], P('tm', None, None, 'space'), may hold values from -6 to 6
- momenta: int32 [16, 3], replicated, may hold values from -2 to 2, as said below
- separations: int32 [4], replicated, may hold values from 1 to 7
Outputs:
- meson: float32 [8, 16, 2, 256, 256], P('tm', 'space')
- correlator: float32 [8, 4, 16, 2], P('tm', None, 'space')
The draws below stay inside these ranges and needn't reach their ends.
Inputs may be any that keep to these rules, and one draw needn't show every extreme that they name: momenta[m + 8] = -momenta[m] for every m below 8.
All inputs are finite; a program needn't handle non-finite values.
Results may differ from the reference program's by a relative error of at most 0.0044.
Values sent between devices are 32-bit elements; how exact they have to be, the bound alone decides.
No kernel may reach another device: no remote copies, remote signals or barrier semaphores. Data moves between devices by JAX's collectives and lax.ppermute only.
A program may use at most 128 MiB of HBM per device.

```python
import math
import jax
import jax.numpy as jnp
from jax import lax

MODES = 256
MOMENTA = 16
OFFSETS = 4
EXTENT = 96
TIMES = 8
SITES = 32768


def draw_momenta(key, part):
    halves = jax.random.randint(jax.random.fold_in(key, 17), (MOMENTA // 2, 3), -2, 3, dtype=jnp.int32)
    return jnp.concatenate([halves, -halves], axis=0)


def touch_ends(array, rng, low, largest):
    longest = array.shape.index(max(array.shape))
    spots = []
    for shift in (0, 1):
        where = [jax.random.randint(jax.random.fold_in(rng, axis), (), 0, length) for axis, length in enumerate(array.shape)]
        where[longest] = (where[longest] + shift) % array.shape[longest]
        spots.append(tuple(where))
    return array.at[spots[0]].set(low).at[spots[1]].set(largest)


def levels(own_key, shape, shards, least, largest):
    factor_of, own = 1.0, jax.random.fold_in(own_key, 6)
    for dim, parts in shards:
        heights = jnp.exp(jax.random.uniform(jax.random.fold_in(own, dim), (parts,), jnp.float32, least / len(shards), largest / len(shards)))
        factor_of = factor_of * jnp.repeat(heights, shape[dim] // parts).reshape([-1 if axis == dim else 1 for axis in range(len(shape))])
    return factor_of


def noise(stream_key, dims, scale, bound, pieces=(), kind=jnp.bfloat16):
    values = scale * jax.random.normal(stream_key, dims, jnp.float32)
    if pieces:
        values = values * levels(stream_key, dims, pieces, -0.22, 0.18)
    return jnp.clip(values, -bound, bound).astype(kind)


def setup_inputs(seed: int = 0) -> dict:
    streams_of = jax.random.split(jax.random.key(seed), 5)
    left_modes = noise(streams_of[0], (TIMES, 2, MODES, SITES), 1.0, 6.0, ((0, 8), (3, 16)))
    right_modes = noise(streams_of[1], (TIMES, 2, MODES, SITES), 1.0, 6.0, ((0, 8), (3, 16)))
    momenta = draw_momenta(jax.random.fold_in(streams_of[4], 71), 0)
    separations = touch_ends(jax.random.randint(streams_of[3], (OFFSETS,), 1, TIMES), jax.random.fold_in(streams_of[3], 1), 1, TIMES - 1).astype(jnp.int32)
    return {"left_modes": left_modes, "right_modes": right_modes, "momenta": momenta, "separations": separations}


def reference(left_modes, right_modes, momenta, separations):
    site_index = jnp.arange(SITES, dtype=jnp.int32)
    x_coord = site_index % EXTENT
    y_coord = site_index // EXTENT % EXTENT
    z_coord = site_index // (EXTENT * EXTENT)

    def one_slice(slice_pair):
        left_slice, right_slice = slice_pair
        right_rows = right_slice.reshape(2 * MODES, SITES)
        left_real = left_slice[0].astype(jnp.float32)
        left_imag = left_slice[1].astype(jnp.float32)

        def one_phase(momentum):
            phase_index = (momentum[0] * x_coord + momentum[1] * y_coord + momentum[2] * z_coord) % EXTENT
            angles = phase_index.astype(jnp.float32) * (2.0 * math.pi / EXTENT)
            cosine = jnp.cos(angles)
            sine_part = jnp.sin(angles)
            phased_real = left_real * cosine - left_imag * sine_part
            phased_imag = -(left_real * sine_part + left_imag * cosine)
            left_rows = jnp.concatenate([phased_real, phased_imag], axis=0).astype(jnp.bfloat16)
            blocks = lax.dot_general(left_rows, right_rows, (((1,), (1,)), ((), ())), preferred_element_type=jnp.float32)
            field_real = blocks[:MODES, :MODES] - blocks[MODES:, MODES:]
            field_imag = blocks[:MODES, MODES:] + blocks[MODES:, :MODES]
            return jnp.stack([field_real, field_imag])
        return lax.map(one_phase, momenta)
    fields = lax.map(one_slice, (left_modes, right_modes))
    meson = fields * jnp.float32(1.0 / math.sqrt(SITES))
    partner_index = (jnp.arange(MOMENTA, dtype=jnp.int32) + MOMENTA // 2) % MOMENTA
    later_fields = jnp.take(meson, partner_index, axis=1)
    transposed = jnp.swapaxes(meson, -1, -2)
    results = []
    for offset in range(OFFSETS):
        targets = (jnp.arange(TIMES, dtype=jnp.int32) + separations[offset]) % TIMES
        chosen = jnp.take(later_fields, targets, axis=0)
        hp = lax.Precision.HIGHEST
        real_part = jnp.einsum('tpij,tpij->tp', transposed[:, :, 0], chosen[:, :, 0], precision=hp) - jnp.einsum('tpij,tpij->tp', transposed[:, :, 1], chosen[:, :, 1], precision=hp)
        imag_part = jnp.einsum('tpij,tpij->tp', transposed[:, :, 0], chosen[:, :, 1], precision=hp) + jnp.einsum('tpij,tpij->tp', transposed[:, :, 1], chosen[:, :, 0], precision=hp)
        results.append(jnp.stack([real_part, imag_part], axis=-1))
    correlator = jnp.stack(results, axis=1) * jnp.float32(1.0 / MODES)
    return (meson, correlator)
```

```python
import functools
import math

import jax
import jax.numpy as jnp
from jax import lax
from jax.experimental import pallas as pl
from jax.experimental.pallas import tpu as pltpu
from jax.sharding import Mesh, PartitionSpec as P

EXTENT = 96
SPACE = ("yh", "yl", "z", "c")
GROUP = ("tm", "yh")


def pair_kernel(row, norm, left_ref, right_ref, cos_ref, sin_ref, out_ref, phased):
    modes = left_ref.shape[1]
    half = modes // 2
    cosine = cos_ref[pl.ds(row, 1), :]
    sine = sin_ref[pl.ds(row, 1), :]
    left_real = left_ref[0].astype(jnp.float32)
    left_imag = left_ref[1].astype(jnp.float32)
    rc, ics = left_real * cosine, left_imag * sine
    rs, ic = left_real * sine, left_imag * cosine
    phased[0 * modes : 1 * modes] = (rc - ics).astype(jnp.bfloat16)
    phased[1 * modes : 2 * modes] = (-(rs + ic)).astype(jnp.bfloat16)
    phased[2 * modes : 3 * modes] = (rc + ics).astype(jnp.bfloat16)
    phased[3 * modes : 4 * modes] = (rs - ic).astype(jnp.bfloat16)
    contract = (((1,), (1,)), ((), ()))
    rows = right_ref[...].reshape(2 * modes, right_ref.shape[2])
    for sign in range(2):
        blocks = lax.dot_general(
            phased[2 * sign * modes : 2 * (sign + 1) * modes], rows, contract, preferred_element_type=jnp.float32
        )
        real = (blocks[:modes, :modes] - blocks[modes:, modes:]) * norm
        imag = (blocks[:modes, modes:] + blocks[modes:, :modes]) * norm
        for part in range(2):
            out_ref[sign, part, 0] = real[part * half : (part + 1) * half]
            out_ref[sign, part, 1] = imag[part * half : (part + 1) * half]


def pair_fields(row, norm, left, right, cosine, sine):
    _, modes, sites = left.shape
    return pl.pallas_call(
        functools.partial(pair_kernel, row, norm),
        out_shape=jax.ShapeDtypeStruct((2, 2, 2, modes // 2, modes), jnp.float32),
        in_specs=[pl.BlockSpec(memory_space=pltpu.VMEM)] * 4,
        out_specs=pl.BlockSpec(memory_space=pltpu.VMEM),
        scratch_shapes=[pltpu.VMEM((4 * modes, sites), jnp.bfloat16)],
        cost_estimate=pl.CostEstimate(
            flops=2 * 4 * modes * 2 * modes * sites, transcendentals=0, bytes_accessed=8 * modes * sites + 8 * modes * modes * 4
        ),
        compiler_params=pltpu.CompilerParams(vmem_limit_bytes=40 * 2**20),
        name=f"pair{row}",
    )(left, right, cosine, sine)


def finish_kernel(flip_ref, own_a, own_b, got_a, got_b, meson_ref, send_ref):
    half = own_a.shape[1]
    peers, _, rows, modes = send_ref.shape
    for c in range(2):
        meson_ref[c, :half] = own_a[c] + got_a[c]
        meson_ref[c, half:] = own_b[c] + got_b[c]

    @pl.when(flip_ref[0] == 0)
    def _():
        for c in range(2):
            send_ref[:, c] = meson_ref[c].reshape(peers, rows, modes)

    @pl.when(flip_ref[0] != 0)
    def _():
        for c in range(2):
            send_ref[:, c] = meson_ref[c].T.reshape(peers, rows, modes)


def gram_kernel(fields_ref, out_ref):
    times = fields_ref.shape[0] // 2
    rows, modes = fields_ref.shape[2:]

    def fold(block):
        total = block[:8]
        for r in range(8, rows, 8):
            total = total + block[r : r + 8]
        lanes = total[:, :128]
        for r in range(128, modes, 128):
            lanes = lanes + total[:, r : r + 128]
        return jnp.sum(lanes, axis=0, keepdims=True)

    for t in range(times):
        x_real, x_imag = fields_ref[2 * t, 0], fields_ref[2 * t, 1]
        for u in range(times):
            y_real, y_imag = fields_ref[2 * u + 1, 0], fields_ref[2 * u + 1, 1]
            real = fold(x_real * y_real - x_imag * y_imag)
            imag = fold(x_real * y_imag + x_imag * y_real)
            out_ref[2 * t, 2 * u : 2 * u + 1] = real
            out_ref[2 * t, 2 * u + 1 : 2 * u + 2] = imag
            out_ref[2 * u + 1, 2 * t : 2 * t + 1] = real
            out_ref[2 * u + 1, 2 * t + 1 : 2 * t + 2] = imag


def along_y(block, step):
    return lax.ppermute(block, ("yh", "yl"), [(y, (y + step) % 4) for y in range(4)])


def swap(block, axis):
    return lax.ppermute(block, axis, [(0, 1), (1, 0)])


def shards(left_modes, right_modes, momenta, separations):
    _, _, modes, sites_dev = left_modes.shape
    left, right = left_modes[0], right_modes[0]
    space_rank = lax.axis_index(SPACE)
    y, z, c = space_rank // 4, space_rank // 2 % 2, space_rank % 2
    site_index = space_rank * sites_dev + jnp.arange(sites_dev, dtype=jnp.int32)
    x_coord = site_index % EXTENT
    y_coord = site_index // EXTENT % EXTENT
    z_coord = site_index // (EXTENT * EXTENT)
    norm = 1.0 / math.sqrt(sites_dev * 16)

    slot = jnp.arange(8, dtype=jnp.int32)
    target = (y + slot // 4) % 4 * 4 + (z ^ (slot // 2 % 2)) * 2 + (c ^ (slot % 2))
    chosen = (target[:, None] == jnp.arange(16, dtype=jnp.int32)[None, :]).astype(jnp.int32)
    momentum = jnp.sum(chosen[:, :, None] * momenta[None], axis=1)
    phase_index = (
        momentum[:, 0:1] * x_coord[None] + momentum[:, 1:2] * y_coord[None] + momentum[:, 2:3] * z_coord[None]
    ) % EXTENT
    angles = phase_index.astype(jnp.float32) * (2.0 * math.pi / EXTENT)
    cosine, sine = jnp.cos(angles), jnp.sin(angles)

    def chip_pair(dy, dz):
        row = 4 * dy + 2 * dz
        other = pair_fields(row + 1, norm, left, right, cosine, sine)
        got = swap(other, "c")
        mine = pair_fields(row, norm, left, right, cosine, sine)
        return mine + got

    held = {}
    for dy, dz in ((1, 1), (1, 0), (0, 1), (0, 0)):
        both = chip_pair(dy, dz)
        held[dy, dz], held[dy + 2, dz] = both[0], both[1]

    reduced = {}
    for dz in (1, 0):
        a = along_y(held[3, dz][0], 1)
        b = along_y(held[1, dz][1], -1)
        a = along_y(a + held[2, dz][0], 1)
        b = along_y(b + held[2, dz][1], -1)
        a = along_y(a + held[1, dz][0], 1)
        b = along_y(b + held[3, dz][1], -1)
        reduced[dz] = (a + held[0, dz][0], b + held[0, dz][1])
    got = [swap(block, "z") for block in reduced[1]]

    flip = lax.axis_index("yh").reshape(1)
    meson, send = pl.pallas_call(
        finish_kernel,
        out_shape=(
            jax.ShapeDtypeStruct((2, modes, modes), jnp.float32),
            jax.ShapeDtypeStruct((16, 2, modes // 16, modes), jnp.float32),
        ),
        in_specs=[pl.BlockSpec(memory_space=pltpu.SMEM)] + [pl.BlockSpec(memory_space=pltpu.VMEM)] * 4,
        out_specs=(pl.BlockSpec(memory_space=pltpu.VMEM),) * 2,
        compiler_params=pltpu.CompilerParams(vmem_limit_bytes=8 * 2**20),
        name="finish",
    )(flip, *reduced[0], *got)

    fields = lax.all_to_all(send, GROUP, 0, 0, tiled=True)
    traces = pl.pallas_call(
        gram_kernel,
        out_shape=jax.ShapeDtypeStruct((16, 16, 128), jnp.float32),
        in_specs=[pl.BlockSpec(memory_space=pltpu.VMEM)],
        out_specs=pl.BlockSpec(memory_space=pltpu.VMEM),
        compiler_params=pltpu.CompilerParams(vmem_limit_bytes=4 * 2**20),
        name="gram",
    )(fields)
    gathered = lax.all_to_all(traces, GROUP, 0, 0, tiled=True)
    own = jnp.sum(gathered, axis=(0, 2)).reshape(8, 2)
    wanted = (lax.axis_index("tm") + separations) % 8
    picked = (wanted[:, None] == jnp.arange(8, dtype=jnp.int32)[None, :]).astype(jnp.float32)
    correlator = jnp.sum(picked[:, :, None] * own[None], axis=1) * jnp.float32(1.0 / modes)
    return meson[None, None], correlator[None, :, None, :]


def solution(mesh):
    fine = Mesh(mesh.devices.reshape(8, 2, 2, 2, 2), ("tm",) + SPACE)
    placed = (P("tm", None, None, SPACE), P("tm", None, None, SPACE), P(), P())
    return jax.shard_map(
        shards,
        mesh=fine,
        in_specs=placed,
        out_specs=(P("tm", SPACE, None, None, None), P("tm", None, SPACE, None)),
        check_vma=False,
    )
```

```python
import functools
import math

import jax
import jax.numpy as jnp
from jax import lax
from jax.experimental import pallas as pl
from jax.experimental.pallas import tpu as pltpu
from jax.sharding import Mesh, PartitionSpec as P


EXTENT = 96
SPACE = ("yh", "yl", "z", "c")
GROUP = ("tm", "yh")
PARTS = ("a", "b", "c", "d")
BLOCKS = {
    "1": (
        ("31c", "11d"), ("11c", "31d"), ("31a", "30a"), ("11b", "10b"), ("11a", "10a"), ("31b", "30b"),
        ("30c",), ("10d",), ("10c",), ("30d",),
    ),
    "2": (("21c", "21d"), ("21a", "20a"), ("21b", "20b"), ("20c",), ("20d",)),
    "3": (("01c", "01d"), ("01a", "01b")),
    "0": (("00a", "00b", "00c", "00d"),),
}


def head_kernel(rank_ref, momenta_ref, left_ref, right_ref, left_out, right_out, cos_ref, sin_ref, sems):
    copies = []
    modes = left_ref.shape[1]
    for source, target in ((right_ref, right_out), (left_ref, left_out)):
        for k in range(4):
            where = (k // 2, pl.ds(k % 2 * (modes // 2), modes // 2))
            copy = pltpu.make_async_copy(source.at[where], target.at[where], sems.at[len(copies)])
            copy.start()
            copies.append(copy)
    rank = rank_ref[0]
    sites = cos_ref.shape[1]
    site = (rank * sites + lax.broadcasted_iota(jnp.int32, (8, sites), 1)).astype(jnp.float32)
    row = lax.broadcasted_iota(jnp.int32, (8, sites), 0)
    lines = jnp.floor((site + 0.5) * (1.0 / EXTENT))
    planes = jnp.floor((lines + 0.5) * (1.0 / EXTENT))
    coords = (site - EXTENT * lines, lines - EXTENT * planes, planes)
    phase = jnp.zeros((8, sites), jnp.float32)
    for axis in range(3):
        component = jnp.zeros((8, sites), jnp.int32)
        for r in range(8):
            across = rank % 4 ^ (r % 4)
            owner = (rank // 4 + r // 4) % 4 * 4 + across
            component = jnp.where(row == r, momenta_ref[axis, owner], component)
        phase = phase + component.astype(jnp.float32) * coords[axis]
    phase = phase - EXTENT * jnp.floor((phase + 0.5) * (1.0 / EXTENT))
    angles = phase * (2.0 * math.pi / EXTENT)
    cos_ref[...] = jnp.cos(angles)
    sin_ref[...] = jnp.sin(angles)
    for copy in copies:
        copy.wait()


def head(rank, momenta, left, right):
    vmem, smem = pl.BlockSpec(memory_space=pltpu.VMEM), pl.BlockSpec(memory_space=pltpu.SMEM)
    hbm = pl.BlockSpec(memory_space=pltpu.HBM)
    table = jax.ShapeDtypeStruct((8, left.shape[2]), jnp.float32)
    return pl.pallas_call(
        head_kernel,
        out_shape=(left, right, table, table),
        in_specs=[smem, smem, hbm, hbm],
        out_specs=(vmem,) * 4,
        scratch_shapes=[pltpu.SemaphoreType.DMA((8,))],
        compiler_params=pltpu.CompilerParams(vmem_limit_bytes=16 * 2**20),
        name="head",
    )(rank.reshape(1), momenta.T, *(pltpu.with_memory_space_constraint(x, pltpu.HBM) for x in (left, right)))


def fields_kernel(units, blocks_of, norm, left_ref, right_ref, cos_ref, sin_ref, out_ref, phased):
    modes = left_ref.shape[1]
    size = out_ref.shape[2]
    rows = right_ref[...].reshape(2 * modes, right_ref.shape[2])
    left_real = left_ref[0].astype(jnp.float32)
    left_imag = left_ref[1].astype(jnp.float32)
    slot = 0
    for row, outs in units:
        cosine = cos_ref[pl.ds(row, 1), :]
        sine = sin_ref[pl.ds(row, 1), :]
        rc, ics = left_real * cosine, left_imag * sine
        rs, ic = left_real * sine, left_imag * cosine
        for sign, name in outs:
            base = slot * 2 * modes
            slot += 1
            real, imag = (rc - ics, -(rs + ic)) if sign > 0 else (rc + ics, rs - ic)
            phased[base : base + modes] = real.astype(jnp.bfloat16)
            phased[base + modes : base + 2 * modes] = imag.astype(jnp.bfloat16)
            sums = lax.dot_general(
                phased[base : base + 2 * modes], rows, (((1,), (1,)), ((), ())), preferred_element_type=jnp.float32
            )
            real = (sums[:modes, :modes] - sums[modes:, modes:]) * norm
            imag = (sums[:modes, modes:] + sums[modes:, :modes]) * norm
            for part, letter in enumerate(PARTS):
                block = blocks_of.index(name + letter)
                out_ref[block, 0] = real[part * size : (part + 1) * size]
                out_ref[block, 1] = imag[part * size : (part + 1) * size]


def fields_of(units, blocks_of, norm, left, right, cosine, sine):
    _, modes, sites = left.shape
    count = sum(len(outs) for _, outs in units)
    return pl.pallas_call(
        functools.partial(fields_kernel, units, blocks_of, norm),
        out_shape=jax.ShapeDtypeStruct((4 * count, 2, modes // 4, modes), jnp.float32),
        in_specs=[pl.BlockSpec(memory_space=pltpu.VMEM)] * 4,
        out_specs=pl.BlockSpec(memory_space=pltpu.VMEM),
        scratch_shapes=[pltpu.VMEM((count * 2 * modes, sites), jnp.bfloat16)],
        cost_estimate=pl.CostEstimate(
            flops=2 * 2 * modes * 2 * modes * sites * count,
            transcendentals=0,
            bytes_accessed=8 * modes * sites + 8 * modes * modes * count,
        ),
        compiler_params=pltpu.CompilerParams(vmem_limit_bytes=36 * 2**20),
        name="fields",
    )(left, right, cosine, sine)


def add_kernel(near_ref, got_ref, *outs):
    start = 0
    for out_ref in outs:
        count = out_ref.shape[0]
        out_ref[...] = near_ref[start : start + count] + got_ref[start : start + count]
        start += count


def add_parts(near, got, counts):
    return pl.pallas_call(
        add_kernel,
        out_shape=tuple(jax.ShapeDtypeStruct((count,) + near.shape[1:], near.dtype) for count in counts),
        in_specs=[pl.BlockSpec(memory_space=pltpu.VMEM)] * 2,
        out_specs=(pl.BlockSpec(memory_space=pltpu.VMEM),) * len(counts),
        compiler_params=pltpu.CompilerParams(vmem_limit_bytes=4 * 2**20),
        name="parts",
    )(near, got)


def turn_kernel(c_ref, d_ref, across_ref, c_own, d_own, c_out, d_out):
    c_out[...] = c_ref[...] + (across_ref[0:1] + c_own[...])
    d_out[...] = d_ref[...] + (across_ref[1:2] + d_own[...])


def turn(c, d, across, c_own, d_own):
    vmem = pl.BlockSpec(memory_space=pltpu.VMEM)
    return pl.pallas_call(
        turn_kernel,
        out_shape=(jax.ShapeDtypeStruct(c.shape, c.dtype),) * 2,
        in_specs=[vmem] * 5,
        out_specs=(vmem, vmem),
        compiler_params=pltpu.CompilerParams(vmem_limit_bytes=2 * 2**20),
        name="turn",
    )(c, d, across, c_own, d_own)


def finish_kernel(flip_ref, own, y_a, y_b, z_ab, y_c, y_d, z_cd, meson_ref, send_ref):
    peers, _, slice_rows, modes = send_ref.shape
    size = own.shape[2]
    for k in range(2):
        meson_ref[k, :size] = y_a[1, k] + own[0, k] + z_ab[0, k]
        meson_ref[k, size : 2 * size] = y_b[1, k] + own[1, k] + z_ab[1, k]
        meson_ref[k, 2 * size : 3 * size] = y_c[0, k] + own[2, k] + z_cd[0, k]
        meson_ref[k, 3 * size :] = y_d[0, k] + own[3, k] + z_cd[1, k]

    @pl.when(flip_ref[0] == 0)
    def _():
        for k in range(2):
            send_ref[:, k] = meson_ref[k].reshape(peers, slice_rows, modes)

    @pl.when(flip_ref[0] != 0)
    def _():
        for k in range(2):
            send_ref[:, k] = meson_ref[k].T.reshape(peers, slice_rows, modes)


def gram_kernel(fields_ref, out_ref, lanes_ref):
    times = fields_ref.shape[0] // 2
    rows, modes = fields_ref.shape[2:]

    def fold(block):
        total = block[:8]
        for r in range(8, rows, 8):
            total = total + block[r : r + 8]
        lanes = total[:, :128]
        for r in range(128, modes, 128):
            lanes = lanes + total[:, r : r + 128]
        return jnp.sum(lanes, axis=0, keepdims=True)

    for t in range(times):
        x_real, x_imag = fields_ref[2 * t, 0], fields_ref[2 * t, 1]
        for u in range(times):
            y_real, y_imag = fields_ref[2 * u + 1, 0], fields_ref[2 * u + 1, 1]
            real = fold(x_real * y_real - x_imag * y_imag)
            imag = fold(x_real * y_imag + x_imag * y_real)
            for row in (32 * t + 2 * u, 32 * u + 16 + 2 * t):
                lanes_ref[row : row + 1] = real
                lanes_ref[row + 1 : row + 2] = imag
    peers = out_ref.shape[0]
    sums = lax.dot_general(
        jnp.ones((peers, 128), jnp.float32), lanes_ref[...], (((1,), (1,)), ((), ())),
        precision=lax.Precision.HIGHEST, preferred_element_type=jnp.float32,
    )
    for p in range(peers):
        out_ref[p] = sums[p : p + 1] * (1.0 / modes)


def along_y(block, step):
    return lax.ppermute(block, ("yh", "yl"), [(y, (y + step) % 4) for y in range(4)])


def swap(block, axis):
    return lax.ppermute(block, axis, [(0, 1), (1, 0)])


def shards(left_modes, right_modes, momenta, separations):
    _, _, modes, sites_dev = left_modes.shape
    norm = 1.0 / math.sqrt(sites_dev * 16)
    tables = head(lax.axis_index(SPACE), momenta, left_modes[0], right_modes[0])

    def chip_sum(name, units):
        blocks_of = [block for group in BLOCKS[name] for block in group]
        far = fields_of(tuple((row + 1, outs) for row, outs in units), blocks_of, norm, *tables)
        got = swap(far, "c")
        near = fields_of(units, blocks_of, norm, *tables)
        return add_parts(near, got, [len(group) for group in BLOCKS[name]])

    z1, z3, a1, b1, a3, b3, c1, d1, c3, d3 = chip_sum("1", ((6, ((-1, "31"), (1, "11"))), (4, ((-1, "30"), (1, "10")))))
    z2, a2, b2, c2, d2 = chip_sum("2", ((2, ((-1, "21"),)), (0, ((-1, "20"),))))
    z4, z5 = chip_sum("3", ((2, ((1, "01"),)),))
    (own,) = chip_sum("0", ((0, ((1, "00"),)),))

    z1 = swap(z1, "z")
    a = along_y(a1, 1)
    b = along_y(b1, -1)
    z3 = swap(z3, "z")
    z2 = swap(z2, "z")
    z4 = swap(z4, "z")
    a = along_y(a + a2, 1)
    b = along_y(b + b2, -1)
    c = along_y(z1[0:1] + c1, 1)
    d = along_y(z1[1:2] + d1, -1)
    a = along_y(a + a3, 1)
    b = along_y(b + b3, -1)
    c, d = turn(c, d, z2, c2, d2)
    c, d = along_y(c, 1), along_y(d, -1)
    z5 = swap(jnp.concatenate([a[0:1], b[0:1]]) + z5, "z")
    c, d = turn(c, d, z3, c3, d3)
    c, d = along_y(c, 1), along_y(d, -1)

    flip = lax.axis_index("yh").reshape(1)
    vmem = pl.BlockSpec(memory_space=pltpu.VMEM)
    meson, send = pl.pallas_call(
        finish_kernel,
        out_shape=(
            jax.ShapeDtypeStruct((2, modes, modes), jnp.float32),
            jax.ShapeDtypeStruct((16, 2, modes // 16, modes), jnp.float32),
        ),
        in_specs=[pl.BlockSpec(memory_space=pltpu.SMEM)] + [vmem] * 7,
        out_specs=(vmem, vmem),
        compiler_params=pltpu.CompilerParams(vmem_limit_bytes=8 * 2**20),
        name="finish",
    )(flip, own, a, b, z5, c, d, z4)

    fields = lax.all_to_all(send, GROUP, 0, 0, tiled=True)
    traces = pl.pallas_call(
        gram_kernel,
        out_shape=jax.ShapeDtypeStruct((16, 1, 256), jnp.float32),
        in_specs=[vmem],
        out_specs=vmem,
        scratch_shapes=[pltpu.VMEM((256, 128), jnp.float32)],
        compiler_params=pltpu.CompilerParams(vmem_limit_bytes=4 * 2**20),
        name="gram",
    )(fields)
    traces = lax.all_to_all(traces, GROUP, 0, 0, tiled=True)
    tm_rank = lax.axis_index("tm")
    wanted = (tm_rank * 2 + lax.axis_index("yh")) * 16 + (tm_rank + separations) % 8 * 2
    lane = jnp.arange(256, dtype=jnp.int32)
    picked = lane[None, None] == wanted[None, :, None] + jnp.arange(2, dtype=jnp.int32)[:, None, None]
    total = jnp.sum(traces[:, 0], axis=0)
    correlator = jnp.sum(jnp.where(picked, total[None, None], 0.0), axis=-1).T
    return meson[None, None], correlator[None, :, None, :]


def solution(mesh):
    fine = Mesh(mesh.devices.reshape(8, 2, 2, 2, 2), ("tm",) + SPACE)
    placed = (P("tm", None, None, SPACE), P("tm", None, None, SPACE), P(), P())

    return jax.shard_map(
        shards,
        mesh=fine,
        in_specs=placed,
        out_specs=(P("tm", SPACE, None, None, None), P("tm", None, SPACE, None)),
        check_vma=False,
    )
```

```python
import functools
import math

import jax
import jax.numpy as jnp
from jax import lax
from jax.experimental import pallas as pl
from jax.experimental.pallas import tpu as pltpu
from jax.sharding import Mesh, PartitionSpec as P


EXTENT = 96
SPACE = ("yh", "yl", "z", "c")
GROUP = ("tm", "yh")
PARTS = ("a", "b", "c", "d")
BLOCKS = {
    "1": (
        ("31c", "11d"), ("11c", "31d"), ("31a", "30a"), ("11b", "10b"), ("11a", "10a"), ("31b", "30b"),
        ("30c",), ("10d",), ("10c",), ("30d",),
    ),
    "2": (("21c", "21d"), ("21a", "20a"), ("21b", "20b"), ("20c",), ("20d",)),
    "3": (("01c", "01d"), ("01a", "01b")),
    "0": (("00a", "00b", "00c", "00d"),),
}


UNITS = {
    "1": ((6, ((-1, "31"), (1, "11"))), (4, ((-1, "30"), (1, "10")))),
    "2": ((2, ((-1, "21"),)), (0, ((-1, "20"),))),
    "3": ((2, ((1, "01"),)),),
    "0": ((0, ((1, "00"),)),),
}


def head_kernel(rank_ref, momenta_ref, left_ref, right_ref, left_out, right_out, cos_ref, sin_ref, sems):
    copies = []
    modes = left_ref.shape[1]
    for source, target in ((right_ref, right_out), (left_ref, left_out)):
        for k in range(4):
            where = (k // 2, pl.ds(k % 2 * (modes // 2), modes // 2))
            copy = pltpu.make_async_copy(source.at[where], target.at[where], sems.at[len(copies)])
            copy.start()
            copies.append(copy)
    rank = rank_ref[0]
    sites = cos_ref.shape[1]
    site = (rank * sites + lax.broadcasted_iota(jnp.int32, (8, sites), 1)).astype(jnp.float32)
    row = lax.broadcasted_iota(jnp.int32, (8, sites), 0)
    lines = jnp.floor((site + 0.5) * (1.0 / EXTENT))
    planes = jnp.floor((lines + 0.5) * (1.0 / EXTENT))
    coords = (site - EXTENT * lines, lines - EXTENT * planes, planes)
    phase = jnp.zeros((8, sites), jnp.float32)
    for axis in range(3):
        component = jnp.zeros((8, sites), jnp.int32)
        for r in range(8):
            across = rank % 4 ^ (r % 4)
            owner = (rank // 4 + r // 4) % 4 * 4 + across
            component = jnp.where(row == r, momenta_ref[axis, owner], component)
        phase = phase + component.astype(jnp.float32) * coords[axis]
    phase = phase - EXTENT * jnp.floor((phase + 0.5) * (1.0 / EXTENT))
    angles = phase * (2.0 * math.pi / EXTENT)
    cos_ref[...] = jnp.cos(angles)
    sin_ref[...] = jnp.sin(angles)
    for copy in copies:
        copy.wait()


def head(rank, momenta, left, right):
    vmem, smem = pl.BlockSpec(memory_space=pltpu.VMEM), pl.BlockSpec(memory_space=pltpu.SMEM)
    hbm = pl.BlockSpec(memory_space=pltpu.HBM)
    table = jax.ShapeDtypeStruct((8, left.shape[2]), jnp.float32)
    return pl.pallas_call(
        head_kernel,
        out_shape=(left, right, table, table),
        in_specs=[smem, smem, hbm, hbm],
        out_specs=(vmem,) * 4,
        scratch_shapes=[pltpu.SemaphoreType.DMA((8,))],
        compiler_params=pltpu.CompilerParams(vmem_limit_bytes=16 * 2**20),
        name="head",
    )(rank.reshape(1), momenta.T, *(pltpu.with_memory_space_constraint(x, pltpu.HBM) for x in (left, right)))


def fields_kernel(units, blocks_of, norm, left_ref, right_ref, cos_ref, sin_ref, out_ref, phased):
    modes = left_ref.shape[1]
    size = out_ref.shape[2]
    rows = right_ref[...].reshape(2 * modes, right_ref.shape[2])
    left_real = left_ref[0].astype(jnp.float32)
    left_imag = left_ref[1].astype(jnp.float32)
    slot = 0
    for row, outs in units:
        cosine = cos_ref[pl.ds(row, 1), :]
        sine = sin_ref[pl.ds(row, 1), :]
        rc, ics = left_real * cosine, left_imag * sine
        rs, ic = left_real * sine, left_imag * cosine
        for sign, name in outs:
            base = slot * 2 * modes
            slot += 1
            real, imag = (rc - ics, -(rs + ic)) if sign > 0 else (rc + ics, rs - ic)
            phased[base : base + modes] = real.astype(jnp.bfloat16)
            phased[base + modes : base + 2 * modes] = imag.astype(jnp.bfloat16)
            sums = lax.dot_general(
                phased[base : base + 2 * modes], rows, (((1,), (1,)), ((), ())), preferred_element_type=jnp.float32
            )
            real = (sums[:modes, :modes] - sums[modes:, modes:]) * norm
            imag = (sums[:modes, modes:] + sums[modes:, :modes]) * norm
            for part, letter in enumerate(PARTS):
                block = blocks_of.index(name + letter)
                out_ref[block, 0] = real[part * size : (part + 1) * size]
                out_ref[block, 1] = imag[part * size : (part + 1) * size]


def fields_of(units, blocks_of, norm, left, right, cosine, sine):
    _, modes, sites = left.shape
    count = sum(len(outs) for _, outs in units)
    return pl.pallas_call(
        functools.partial(fields_kernel, units, blocks_of, norm),
        out_shape=jax.ShapeDtypeStruct((4 * count, 2, modes // 4, modes), jnp.float32),
        in_specs=[pl.BlockSpec(memory_space=pltpu.VMEM)] * 4,
        out_specs=pl.BlockSpec(memory_space=pltpu.VMEM),
        scratch_shapes=[pltpu.VMEM((count * 2 * modes, sites), jnp.bfloat16)],
        cost_estimate=pl.CostEstimate(
            flops=2 * 2 * modes * 2 * modes * sites * count,
            transcendentals=0,
            bytes_accessed=8 * modes * sites + 8 * modes * modes * count,
        ),
        compiler_params=pltpu.CompilerParams(vmem_limit_bytes=36 * 2**20),
        name="fields",
    )(left, right, cosine, sine)


def add_kernel(skip, near_ref, got_ref, *outs):
    start = 0
    for out_ref in outs:
        count = out_ref.shape[0]
        out_ref[...] = near_ref[start : start + count] + got_ref[skip + start : skip + start + count]
        start += count


def add_parts(near, got, counts, skip):
    return pl.pallas_call(
        functools.partial(add_kernel, skip),
        out_shape=tuple(jax.ShapeDtypeStruct((count,) + near.shape[1:], near.dtype) for count in counts),
        in_specs=[pl.BlockSpec(memory_space=pltpu.VMEM)] * 2,
        out_specs=(pl.BlockSpec(memory_space=pltpu.VMEM),) * len(counts),
        compiler_params=pltpu.CompilerParams(vmem_limit_bytes=4 * 2**20),
        name="parts",
    )(near, got)


def turn_kernel(c_ref, d_ref, across_ref, c_own, d_own, c_out, d_out):
    c_out[...] = c_ref[...] + (across_ref[0:1] + c_own[...])
    d_out[...] = d_ref[...] + (across_ref[1:2] + d_own[...])


def turn(c, d, across, c_own, d_own):
    vmem = pl.BlockSpec(memory_space=pltpu.VMEM)
    return pl.pallas_call(
        turn_kernel,
        out_shape=(jax.ShapeDtypeStruct(c.shape, c.dtype),) * 2,
        in_specs=[vmem] * 5,
        out_specs=(vmem, vmem),
        compiler_params=pltpu.CompilerParams(vmem_limit_bytes=2 * 2**20),
        name="turn",
    )(c, d, across, c_own, d_own)


def finish_kernel(flip_ref, own, y_a, y_b, z_ab, y_c, y_d, z_cd, meson_ref, send_ref):
    peers, _, slice_rows, modes = send_ref.shape
    size = own.shape[2]
    for k in range(2):
        meson_ref[k, :size] = y_a[1, k] + own[0, k] + z_ab[0, k]
        meson_ref[k, size : 2 * size] = y_b[1, k] + own[1, k] + z_ab[1, k]
        meson_ref[k, 2 * size : 3 * size] = y_c[0, k] + own[2, k] + z_cd[0, k]
        meson_ref[k, 3 * size :] = y_d[0, k] + own[3, k] + z_cd[1, k]

    @pl.when(flip_ref[0] == 0)
    def _():
        for k in range(2):
            send_ref[:, k] = meson_ref[k].reshape(peers, slice_rows, modes)

    @pl.when(flip_ref[0] != 0)
    def _():
        for k in range(2):
            send_ref[:, k] = meson_ref[k].T.reshape(peers, slice_rows, modes)


def gram_kernel(fields_ref, out_ref, lanes_ref):
    times = fields_ref.shape[0] // 2
    rows, modes = fields_ref.shape[2:]

    def fold(block):
        total = block[:8]
        for r in range(8, rows, 8):
            total = total + block[r : r + 8]
        lanes = total[:, :128]
        for r in range(128, modes, 128):
            lanes = lanes + total[:, r : r + 128]
        return jnp.sum(lanes, axis=0, keepdims=True)

    for t in range(times):
        x_real, x_imag = fields_ref[2 * t, 0], fields_ref[2 * t, 1]
        for u in range(times):
            y_real, y_imag = fields_ref[2 * u + 1, 0], fields_ref[2 * u + 1, 1]
            real = fold(x_real * y_real - x_imag * y_imag)
            imag = fold(x_real * y_imag + x_imag * y_real)
            for row in (32 * t + 2 * u, 32 * u + 16 + 2 * t):
                lanes_ref[row : row + 1] = real
                lanes_ref[row + 1 : row + 2] = imag
    peers = out_ref.shape[0]
    sums = lax.dot_general(
        jnp.ones((8, 128), jnp.float32), lanes_ref[...], (((1,), (1,)), ((), ())),
        precision=lax.Precision.HIGHEST, preferred_element_type=jnp.float32,
    )
    row = sums[0:1] * (1.0 / modes)
    for p in range(peers):
        out_ref[p] = row


def along_y(block, step):
    return lax.ppermute(block, ("yh", "yl"), [(y, (y + step) % 4) for y in range(4)])


def swap(block, axis):
    return lax.ppermute(block, axis, [(0, 1), (1, 0)])


def shards(left_modes, right_modes, momenta, separations):
    _, _, modes, sites_dev = left_modes.shape
    norm = 1.0 / math.sqrt(sites_dev * 16)
    tables = head(lax.axis_index(SPACE), momenta, left_modes[0], right_modes[0])

    def names(slots):
        return [block for slot in slots for group in BLOCKS[slot] for block in group]

    def far_fields(slots):
        units = tuple((row + 1, outs) for slot in slots for row, outs in UNITS[slot])
        far = fields_of(units, names(slots), norm, *tables)
        return swap(far, "c")

    def chip_sum(slot, got, skip=0):
        near = fields_of(UNITS[slot], names(slot), norm, *tables)
        return add_parts(near, got, [len(group) for group in BLOCKS[slot]], skip)

    z1, z3, a1, b1, a3, b3, c1, d1, c3, d3 = chip_sum("1", far_fields("1"))
    got = far_fields("23")
    z2, a2, b2, c2, d2 = chip_sum("2", got)
    z4, z5 = chip_sum("3", got, len(names("2")))
    (own,) = chip_sum("0", far_fields("0"))

    z1 = swap(z1, "z")
    a = along_y(a1, 1)
    b = along_y(b1, -1)
    z3 = swap(z3, "z")
    z2 = swap(z2, "z")
    z4 = swap(z4, "z")
    a = along_y(a + a2, 1)
    b = along_y(b + b2, -1)
    c = along_y(z1[0:1] + c1, 1)
    d = along_y(z1[1:2] + d1, -1)
    a = along_y(a + a3, 1)
    b = along_y(b + b3, -1)
    c, d = turn(c, d, z2, c2, d2)
    c, d = along_y(c, 1), along_y(d, -1)
    z5 = swap(jnp.concatenate([a[0:1], b[0:1]]) + z5, "z")
    c, d = turn(c, d, z3, c3, d3)
    c, d = along_y(c, 1), along_y(d, -1)

    flip = lax.axis_index("yh").reshape(1)
    vmem = pl.BlockSpec(memory_space=pltpu.VMEM)
    meson, send = pl.pallas_call(
        finish_kernel,
        out_shape=(
            jax.ShapeDtypeStruct((2, modes, modes), jnp.float32),
            jax.ShapeDtypeStruct((16, 2, modes // 16, modes), jnp.float32),
        ),
        in_specs=[pl.BlockSpec(memory_space=pltpu.SMEM)] + [vmem] * 7,
        out_specs=(vmem, vmem),
        compiler_params=pltpu.CompilerParams(vmem_limit_bytes=8 * 2**20),
        name="finish",
    )(flip, own, a, b, z5, c, d, z4)

    fields = lax.all_to_all(send, GROUP, 0, 0, tiled=True)
    traces = pl.pallas_call(
        gram_kernel,
        out_shape=jax.ShapeDtypeStruct((16, 1, 256), jnp.float32),
        in_specs=[vmem],
        out_specs=vmem,
        scratch_shapes=[pltpu.VMEM((256, 128), jnp.float32)],
        compiler_params=pltpu.CompilerParams(vmem_limit_bytes=4 * 2**20),
        name="gram",
    )(fields)
    traces = lax.all_to_all(traces, GROUP, 0, 0, tiled=True)
    tm_rank = lax.axis_index("tm")
    wanted = (tm_rank * 2 + lax.axis_index("yh")) * 16 + (tm_rank + separations) % 8 * 2
    lane = jnp.arange(256, dtype=jnp.int32)
    picked = lane[None, None] == wanted[None, :, None] + jnp.arange(2, dtype=jnp.int32)[:, None, None]
    total = jnp.sum(traces[:, 0], axis=0)
    correlator = jnp.sum(jnp.where(picked, total[None, None], 0.0), axis=-1).T
    return meson[None, None], correlator[None, :, None, :]


def solution(mesh):
    fine = Mesh(mesh.devices.reshape(8, 2, 2, 2, 2), ("tm",) + SPACE)
    placed = (P("tm", None, None, SPACE), P("tm", None, None, SPACE), P(), P())

    return jax.shard_map(
        shards,
        mesh=fine,
        in_specs=placed,
        out_specs=(P("tm", SPACE, None, None, None), P("tm", None, SPACE, None)),
        check_vma=False,
    )
```
